32 devices in a mesh: gx: 4 (over z), gy: 4 (over y, core), gz: 2 (over x).
Axes of the slice: x: 2, y: 2, z: 4, core: 2. Of those that a mesh axis runs over, the one named last changes fastest.
Arguments:
- positions_now: float32 [32, 16, 2, 4, 128], P('gx', 'gy', 'gz'), may hold values from 0 to 1
- velocities: float32 [32, 16, 2, 3, 128], P('gx', 'gy', 'gz'), may hold values from -6 to 6
- positions_next: float32 [32, 16, 2, 3, 128], P('gx', 'gy', 'gz'), may hold values from 0 to 1
- halo_counts: int32 [32, 16, 2], P('gx', 'gy', 'gz'), may hold values from 1 to 128, as said below
- neighbour_lists: int32 [32, 16, 2, 14], P('gx', 'gy', 'gz'), may hold values from 0 to 26, as said below
- descendants: int32 [32, 16, 2, 2, 128], P('gx', 'gy', 'gz'), may hold values from 0 to 127, as said below
Outputs:
- drift: float32 [32, 16, 2, 3, 128], P('gx', 'gy', 'gz')
- tension: float32 [32, 16, 2, 128], P('gx', 'gy', 'gz')
The draws below stay inside these ranges and needn't reach their ends.
Inputs may be any that keep to these rules, and one draw needn't show every extreme that they name: `halo_counts`: every cell holds 1 to 128 live halos; some cell holds exactly 128. `neighbour_lists`: each cell's list begins with code 13 (the cell itself) and holds distinct codes. `descendants`: row 0 is a code 0 to 26; row 1 is a live slot of the descendant's cell.
All inputs are finite; a program needn't handle non-finite values.
Results may differ from the reference program's by a relative error of at most 0.0003.
Values sent between devices are 32-bit elements; how exact they have to be, the bound alone decides.
A program may use at most 64 MiB of HBM per device.

```python
import jax
import jax.numpy as jnp
from jax import lax

SLOTS = 128
NBR = 14
NX = 32
NY = 16
NZ = 2


def make_counts(key):
    shape = (NX, NY, NZ)
    xpos = jnp.arange(NX, dtype=jnp.int32)[:, None, None]
    upper = 32 + 96 * (xpos + 1) // NX
    raw = jax.random.randint(key, shape, 0, 1 << 20, dtype=jnp.int32)
    counts = 1 + raw % upper
    return counts.at[NX - 1, 0, 0].set(SLOTS)


def draw_halo_counts(key, part):
    return make_counts(jax.random.fold_in(key, 11))


def draw_neighbour_lists(key, part):
    sub = jax.random.fold_in(key, 23)
    scores = jax.random.randint(sub, (NX, NY, NZ, 26), 0, 1 << 20, dtype=jnp.int32) * 32 + jnp.arange(26, dtype=jnp.int32)
    order = jnp.argsort(scores, axis=-1, stable=True)[..., :NBR - 1].astype(jnp.int32)
    codes = jnp.where(order < 13, order, order + 1)
    selfcode = jnp.full((NX, NY, NZ, 1), 13, jnp.int32)
    return jnp.concatenate([selfcode, codes], axis=-1)


def draw_descendants(key, part):
    counts = make_counts(jax.random.fold_in(key, 11))
    sub = jax.random.fold_in(key, 37)
    first, second = jax.random.split(sub)
    codes = jax.random.randint(first, (NX, NY, NZ, SLOTS), 0, 27, dtype=jnp.int32)
    rolled = []
    for code in range(27):
        dx, dy, dz = (code // 9 - 1, code // 3 % 3 - 1, code % 3 - 1)
        rolled.append(jnp.roll(counts, (-dx, -dy, -dz), axis=(0, 1, 2)))
    table = jnp.stack(rolled, axis=-1)
    hits = (codes[..., None] == jnp.arange(27, dtype=jnp.int32)).astype(jnp.int32)
    target_count = jnp.sum(hits * table[:, :, :, None, :], axis=-1)
    raw = jax.random.randint(second, (NX, NY, NZ, SLOTS), 0, 1 << 20, dtype=jnp.int32)
    slotid = raw % target_count
    return jnp.stack([codes, slotid], axis=3)


def shard_levels(rng, extent, pieces, low, largest):
    loudness = 1.0
    for position, parts in pieces:
        heights = jax.random.uniform(jax.random.fold_in(jax.random.fold_in(rng, 6), position), (parts,), jnp.float32, low / len(pieces), largest / len(pieces))
        loudness = loudness * jnp.repeat(jnp.exp(heights), extent[position] // parts).reshape((-1,) + (1,) * (len(extent) - 1 - position))
    return loudness


def noise(own_key, shape, scale, limit, cuts=(), kind=jnp.bfloat16):
    result = scale * jax.random.normal(own_key, shape, jnp.float32)
    if cuts:
        result = result * shard_levels(own_key, shape, cuts, -0.22, 0.18)
    return jnp.clip(result, -limit, limit).astype(kind)


def setup_inputs(seed: int = 0) -> dict:
    splits = jax.random.split(jax.random.key(seed), 7)
    positions_now = jnp.clip(1.0 * jax.random.uniform(splits[0], (NX, NY, NZ, 4, SLOTS), jnp.float32) ** shard_levels(splits[0], (NX, NY, NZ, 4, SLOTS), ((0, 4), (1, 4), (2, 2)), -0.2, 0.2), 0.0, 1.0)
    velocities = noise(splits[1], (NX, NY, NZ, 3, SLOTS), 1.0, 6.0, ((0, 4), (1, 4), (2, 2)), jnp.float32)
    positions_next = jnp.clip(1.0 * jax.random.uniform(splits[2], (NX, NY, NZ, 3, SLOTS), jnp.float32) ** shard_levels(splits[2], (NX, NY, NZ, 3, SLOTS), ((0, 4), (1, 4), (2, 2)), -0.2, 0.2), 0.0, 1.0)
    halo_counts = draw_halo_counts(jax.random.fold_in(splits[6], 71), 0)
    neighbour_lists = draw_neighbour_lists(jax.random.fold_in(splits[6], 71), 0)
    descendants = draw_descendants(jax.random.fold_in(splits[6], 71), 0)
    return {"positions_now": positions_now, "velocities": velocities, "positions_next": positions_next, "halo_counts": halo_counts, "neighbour_lists": neighbour_lists, "descendants": descendants}


EPS_SQ = 0.01
STEP_DT = 0.3
HALF_KICK = 0.045

def offsets_of(code):
    return (code // 9 - 1, code // 3 % 3 - 1, code % 3 - 1)

def stack_state(positions_now, positions_next, halo_counts):
    slots = positions_now.shape[-1]
    live = (jnp.arange(slots, dtype=jnp.int32)[None, None, None, :] < halo_counts[..., None]).astype(jnp.float32)
    masses = positions_now[:, :, :, 3:4, :] * live[:, :, :, None, :]
    return (jnp.concatenate([positions_now[:, :, :, :3, :], masses, positions_next], axis=3), live)

def predict(padded, neighbour_lists, velocities, descendants, halo_counts):
    cx, cy, cz = neighbour_lists.shape[:3]
    width = neighbour_lists.shape[3]
    px, py, pz = (cx + 2, cy + 2, cz + 2)
    slots = padded.shape[-1]
    cells = cx * cy * cz
    flat = padded.reshape(px * py * pz, 7, slots)
    next_rows = jnp.transpose(flat[:, 4:7, :], (0, 2, 1)).reshape(px * py * pz * slots, 3)
    grid = jnp.indices((cx, cy, cz), dtype=jnp.int32).reshape(3, cells)
    base = ((grid[0] + 1) * py + grid[1] + 1) * pz + grid[2] + 1
    group = 32 if cells % 32 == 0 else cells
    blocks = cells // group
    lists = neighbour_lists.reshape(blocks, group, width)
    vel = velocities.reshape(blocks, group, 3, slots)
    desc = descendants.reshape(blocks, group, 2, slots)
    counts = halo_counts.reshape(blocks, group)
    bases = base.reshape(blocks, group)

    def one_group(items):
        base_g, list_g, vel_g, desc_g, count_g = items
        own = flat[base_g]
        pos = own[:, :3, :]

        def step(accel, code):
            dx, dy, dz = offsets_of(code)
            source = flat[base_g + dx * py * pz + dy * pz + dz]
            offset = jnp.stack([dx, dy, dz], 1).astype(jnp.float32)
            spot = offset[:, :, None] + source[:, :3, :]
            diff = spot[:, :, None, :] - pos[:, :, :, None]
            dist_sq = lax.optimization_barrier(jnp.sum(diff * diff, axis=1)) + EPS_SQ
            weight = source[:, 3, None, :] / (dist_sq * jnp.sqrt(dist_sq))
            return (accel + lax.optimization_barrier(jnp.sum(diff * weight[:, None, :, :], axis=3)), None)
        accel, _ = lax.scan(step, jnp.zeros(pos.shape, jnp.float32), jnp.transpose(list_g))
        predicted = pos + STEP_DT * vel_g + HALF_KICK * accel
        dcode = desc_g[:, 0, :]
        dslot = desc_g[:, 1, :]
        ddx, ddy, ddz = offsets_of(dcode)
        target = base_g[:, None] + ddx * py * pz + ddy * pz + ddz
        found = jnp.transpose(next_rows[target * slots + dslot], (0, 2, 1))
        offset = jnp.stack([ddx, ddy, ddz], 1).astype(jnp.float32)
        error = offset + found - predicted
        live = (jnp.arange(slots, dtype=jnp.int32)[None, :] < count_g[:, None]).astype(jnp.float32)
        drift = error * live[:, None, :]
        squared = lax.optimization_barrier(jnp.sum(error * error, axis=1)) * live
        return (drift, squared)
    drift, squared = lax.map(one_group, (bases, lists, vel, desc, counts))
    return (drift.reshape(cx, cy, cz, 3, slots), squared.reshape(cx, cy, cz, slots))

def reference(positions_now, velocities, positions_next, halo_counts, neighbour_lists, descendants):
    state, live = stack_state(positions_now, positions_next, halo_counts)
    padded = jnp.pad(state, ((1, 1), (1, 1), (1, 1), (0, 0), (0, 0)), mode='wrap')
    drift, squared = predict(padded, neighbour_lists, velocities, descendants, halo_counts)
    mean_sq = jnp.sum(squared) / jnp.sum(live)
    return (drift, squared / (mean_sq + 1e-06))
```

```python
import functools

import jax
import jax.numpy as jnp
from jax import lax
from jax.experimental import pallas as pl
from jax.experimental.pallas import tpu as pltpu
from jax.sharding import PartitionSpec as P

EPS_SQ = 0.01
STEP_DT = 0.3
HALF_KICK = 0.045


def shifted(shard, axis, by):
    peers = lax.axis_size(axis)
    return lax.ppermute(shard, axis, [(i, (i + by) % peers) for i in range(peers)])


def pieces(tile):
    first = tile.astype(jnp.bfloat16).astype(jnp.float32)
    rest = tile - first
    second = rest.astype(jnp.bfloat16).astype(jnp.float32)
    return first, second, rest - second


def kernel(dims, width, lists, padded, vel, desc, drift_ref, sq_ref, feat, moment, placed):
    cx, cy, cz = dims
    py, pz = cy + 2, cz + 2
    cells = cx * cy * cz
    slots = padded.shape[-1]
    row = lax.broadcasted_iota(jnp.int32, (8, slots), 0)

    def place(n, _):
        ix, iy, iz = n // (py * pz), n // pz % py, n % pz
        fx = ix.astype(jnp.float32) - (cx + 2) / 2
        fy = iy.astype(jnp.float32) - (cy + 2) / 2
        fz = iz.astype(jnp.float32) - (cz + 2) / 2
        shift = jnp.where(row % 4 == 0, fx, jnp.where(row % 4 == 1, fy, jnp.where(row % 4 == 2, fz, 0.0)))
        tile = padded[n] + shift
        placed[n] = tile
        mass = tile[3:4]
        norm = tile[0:1] * tile[0:1] + tile[1:2] * tile[1:2] + tile[2:3] * tile[2:3]
        ext = jnp.where(row < 3, tile, jnp.where(row == 3, norm, jnp.where(row == 4, 1.0, 0.0)))
        a, b, c = pieces(ext)
        feat[n] = jnp.concatenate([a, a, a, b, b, c], axis=0).astype(jnp.bfloat16)
        mom = jnp.where(row < 3, tile * mass, jnp.where(row == 3, mass, 0.0))
        moment[n] = jnp.concatenate(list(pieces(mom)) + [jnp.zeros_like(mom)], axis=0).astype(jnp.bfloat16)
        return 0

    lax.fori_loop(0, padded.shape[0], place, 0)

    def target(n, _):
        ix, iy, iz = n // (cy * cz), n // cz % cy, n % cz
        corner = (ix * py + iy) * pz + iz
        base = corner + (py + 1) * pz + 1
        own = placed[base]
        norm = own[0:1] * own[0:1] + own[1:2] * own[1:2] + own[2:3] * own[2:3]
        ext = jnp.where(row < 3, -2.0 * own, jnp.where(row == 3, 1.0, jnp.where(row == 4, norm + EPS_SQ, 0.0)))
        a, b, c = pieces(ext)
        lhs = jnp.concatenate([a, b, c, a, b, a], axis=0).T.astype(jnp.bfloat16)

        def source(k):
            code = lists[n * width + k]
            d9 = (code * 57) >> 9
            d3 = (code * 43) >> 7
            return corner + d9 * (py * pz) + (d3 - 3 * d9) * pz + code - 3 * d3

        acc = jnp.zeros((slots, 32), jnp.float32)
        for k in range(0, width, 2):
            cells_k = [source(j) for j in range(k, min(k + 2, width))]
            f = jnp.concatenate([feat[s] for s in cells_k], axis=1)
            z = jnp.concatenate([moment[s] for s in cells_k], axis=1)
            dist_sq = jnp.dot(lhs, f, preferred_element_type=jnp.float32)
            inv = lax.rsqrt(dist_sq)
            weight = inv * inv * inv
            high = weight.astype(jnp.bfloat16)
            low = (weight - high.astype(jnp.float32)).astype(jnp.bfloat16)
            dn = (((1,), (1,)), ((), ()))
            acc += lax.dot_general(high, z, dn, preferred_element_type=jnp.float32)
            acc += lax.dot_general(low, z, dn, preferred_element_type=jnp.float32)
        acc = acc.T
        sums = acc[0:8] + acc[8:16] + acc[16:24]
        accel = sums[0:3] - own[0:3] * sums[3:4]
        predicted = own[0:3] + STEP_DT * vel[n] + HALF_KICK * accel
        links = desc[n]
        dcode = jnp.broadcast_to(links[0:1], (8, slots))
        dslot = jnp.broadcast_to(links[1:2], (8, slots))
        found = jnp.zeros((8, slots), jnp.float32)
        for code in range(27):
            at = corner + (code // 9) * py * pz + (code // 3 % 3) * pz + code % 3
            got = jnp.take_along_axis(placed[at], dslot, axis=1)
            found = jnp.where(dcode == code, got, found)
        error = found[4:7] - predicted
        live = own[7:8]
        drift_ref[n] = error * live
        sq_ref[pl.ds(n, 1), :] = jnp.sum(error * error, axis=0, keepdims=True) * live
        return 0

    lax.fori_loop(0, cells, target, 0)


def shards(positions_now, velocities, positions_next, halo_counts, neighbour_lists, descendants):
    slots = positions_now.shape[-1]
    cx, cy, cz, width = neighbour_lists.shape
    cells = cx * cy * cz
    live = (
        jnp.arange(slots, dtype=jnp.int32)[None, None, None, :] < halo_counts[..., None]
    ).astype(jnp.float32)
    lv = live[:, :, :, None, :]
    state = jnp.concatenate(
        [positions_now[:, :, :, :3, :], positions_now[:, :, :, 3:4, :] * lv, positions_next, lv], axis=3
    )
    below = shifted(state[-1:], "gx", 1)
    above = shifted(state[:1], "gx", -1)
    state = jnp.concatenate([below, state, above], axis=0)
    below = shifted(state[:, -1:], "gy", 1)
    above = shifted(state[:, :1], "gy", -1)
    state = jnp.concatenate([below, state, above], axis=1)
    if lax.axis_size("gz") == 2 and cz == 1:
        below = above = shifted(state, "gz", 1)
    else:
        below = shifted(state[:, :, -1:], "gz", 1)
        above = shifted(state[:, :, :1], "gz", -1)
    padded = jnp.concatenate([below, state, above], axis=2).reshape(-1, 8, slots)
    count = padded.shape[0]
    drift, squared = pl.pallas_call(
        functools.partial(kernel, (cx, cy, cz), width),
        out_shape=(
            jax.ShapeDtypeStruct((cells, 3, slots), jnp.float32),
            jax.ShapeDtypeStruct((cells, slots), jnp.float32),
        ),
        in_specs=[pl.BlockSpec(memory_space=pltpu.SMEM)] + [pl.BlockSpec(memory_space=pltpu.VMEM)] * 3,
        out_specs=(pl.BlockSpec(memory_space=pltpu.VMEM),) * 2,
        scratch_shapes=[
            pltpu.VMEM((count, 48, slots), jnp.bfloat16),
            pltpu.VMEM((count, 32, slots), jnp.bfloat16),
            pltpu.VMEM((count, 8, slots), jnp.float32),
        ],
    )(
        neighbour_lists.reshape(-1),
        padded,
        velocities.reshape(cells, 3, slots),
        descendants.reshape(cells, 2, slots),
    )
    total_sq, total_live = lax.psum((jnp.sum(squared), jnp.sum(live)), ("gx", "gy", "gz"))
    mean_sq = total_sq / total_live
    tension = squared / (mean_sq + 1e-06)
    return (drift.reshape(cx, cy, cz, 3, slots), tension.reshape(cx, cy, cz, slots))


def solution(mesh):
    return jax.shard_map(
        shards,
        mesh=mesh,
        in_specs=(
            P("gx", "gy", "gz", None, None),
            P("gx", "gy", "gz", None, None),
            P("gx", "gy", "gz", None, None),
            P("gx", "gy", "gz"),
            P("gx", "gy", "gz", None),
            P("gx", "gy", "gz", None, None),
        ),
        out_specs=(P("gx", "gy", "gz", None, None), P("gx", "gy", "gz", None)),
        check_vma=False,
    )
```

```python
import functools

import jax
import jax.numpy as jnp
from jax import lax
from jax.experimental import pallas as pl
from jax.experimental.pallas import tpu as pltpu
from jax.sharding import PartitionSpec as P

EPS_SQ = 0.01
STEP_DT = 0.3
HALF_KICK = 0.045
SPAN = 4


def shifted(shard, axis, by):
    peers = lax.axis_size(axis)
    return lax.ppermute(shard, axis, [(i, (i + by) % peers) for i in range(peers)])


def pieces(tile):
    first = tile.astype(jnp.bfloat16).astype(jnp.float32)
    rest = tile - first
    second = rest.astype(jnp.bfloat16).astype(jnp.float32)
    return first, second, rest - second


def kernel(dims, width, lists, counts, padded, vel, desc, drift_ref, sq_ref, stat_ref, placed, packed):
    cx, cy, cz = dims
    py, pz = cy + 2, cz + 2
    cells = cx * cy * cz
    slots = padded.shape[-1]
    row = lax.broadcasted_iota(jnp.int32, (8, slots), 0)
    lane = lax.broadcasted_iota(jnp.int32, (8, slots), 1)
    wide = SPAN * slots
    wrow = lax.broadcasted_iota(jnp.int32, (8, wide), 0)

    def place(n, _):
        ix, iy, iz = n // (py * pz), n // pz % py, n % pz
        fx = ix.astype(jnp.float32) - (cx + 2) / 2
        fy = iy.astype(jnp.float32) - (cy + 2) / 2
        fz = iz.astype(jnp.float32) - (cz + 2) / 2
        shift = jnp.where(row % 4 == 0, fx, jnp.where(row % 4 == 1, fy, jnp.where(row % 4 == 2, fz, 0.0)))
        placed[n] = padded[n] + shift
        return 0

    lax.fori_loop(0, padded.shape[0], place, 0, unroll=4)

    def target(n, stats):
        ix, iy, iz = n // (cy * cz), n // cz % cy, n % cz
        corner = (ix * py + iy) * pz + iz
        base = corner + (py + 1) * pz + 1
        own = placed[base]
        count = counts[base]

        def source(k):
            code = lists[n * width + k]
            d9 = (code * 57) >> 9
            d3 = (code * 43) >> 7
            return corner + d9 * (py * pz) + (d3 - 3 * d9) * pz + code - 3 * d3

        at = jnp.int32(0)
        for k in range(width):
            cell = source(k)
            q, by = at // slots, at % slots
            turned = pltpu.roll(placed[cell], by, 1)
            packed[q] = jnp.where(lane >= by, turned, packed[q])
            packed[q + 1] = turned
            at = at + counts[cell]
        q, by = at // slots, at % slots
        packed[q] = jnp.where(lane >= by, 0.0, packed[q])
        for k in range(1, SPAN):
            packed[q + k] = jnp.zeros_like(own)
        chunks = (at + wide - 1) // wide

        norm = own[0:1] * own[0:1] + own[1:2] * own[1:2] + own[2:3] * own[2:3]
        ext = jnp.where(row < 3, -2.0 * own, jnp.where(row == 3, 1.0, jnp.where(row == 4, norm + EPS_SQ, 0.0)))
        a, b, c = pieces(ext)
        lhs = jnp.concatenate([a, b, c, a, b, a], axis=0).T.astype(jnp.bfloat16)

        def chunk(rows, m, acc):
            tile = jnp.concatenate([packed[m * SPAN + k] for k in range(SPAN)], axis=1)
            mass = tile[3:4]
            size = tile[0:1] * tile[0:1] + tile[1:2] * tile[1:2] + tile[2:3] * tile[2:3]
            x = jnp.where(wrow < 3, tile, jnp.where(wrow == 3, size, jnp.where(wrow == 4, 1.0, 0.0)))
            a, b, c = pieces(x)
            f = jnp.concatenate([a, a, a, b, b, c], axis=0).astype(jnp.bfloat16)
            mom = jnp.where(wrow < 3, tile * mass, jnp.where(wrow == 3, mass, 0.0))
            z = jnp.concatenate(list(pieces(mom)) + [jnp.zeros_like(mom)], axis=0).astype(jnp.bfloat16)
            dist_sq = jnp.dot(lhs[:rows], f, preferred_element_type=jnp.float32)
            inv = lax.rsqrt(dist_sq)
            weight = inv * inv * inv
            high = weight.astype(jnp.bfloat16)
            low = (weight - high.astype(jnp.float32)).astype(jnp.bfloat16)
            dn = (((1,), (1,)), ((), ()))
            acc += lax.dot_general(high, z, dn, preferred_element_type=jnp.float32)
            acc += lax.dot_general(low, z, dn, preferred_element_type=jnp.float32)
            return acc

        def attract(rows):
            acc = lax.fori_loop(
                0, chunks, functools.partial(chunk, rows), jnp.zeros((rows, 32), jnp.float32)
            )
            if rows < slots:
                acc = jnp.concatenate([acc, jnp.zeros((slots - rows, 32), jnp.float32)], axis=0)
            return acc

        acc = lax.cond(count > slots // 2, lambda: attract(slots), lambda: attract(slots // 2))
        acc = acc.T
        sums = acc[0:8] + acc[8:16] + acc[16:24]
        accel = sums[0:3] - own[0:3] * sums[3:4]
        predicted = own[0:3] + STEP_DT * vel[n] + HALF_KICK * accel
        links = desc[n]
        dcode = jnp.broadcast_to(links[0:1], (8, slots))
        dslot = jnp.broadcast_to(links[1:2], (8, slots))
        found = jnp.zeros((8, slots), jnp.float32)
        for code in range(27):
            near = corner + (code // 9) * py * pz + (code // 3 % 3) * pz + code % 3
            got = jnp.take_along_axis(placed[near], dslot, axis=1)
            found = jnp.where(dcode == code, got, found)
        live = lane[0:1] < count
        error = jnp.where(live, found[4:7] - predicted, 0.0)
        drift_ref[n] = error
        squared = jnp.sum(error * error, axis=0, keepdims=True)
        sq_ref[pl.ds(n, 1), :] = squared
        return stats + jnp.where(row == 0, squared, jnp.where((row == 1) & live, 1.0, 0.0))

    stat_ref[...] = lax.fori_loop(0, cells, target, jnp.zeros((8, slots), jnp.float32))


def scale_kernel(axes, sizes, stat, squared, out, inbox, send_sem, recv_sem):
    total = 1
    me = 0
    for name, size in zip(axes, sizes):
        total *= size
        me = me * size + lax.axis_index(name)

    def peer(step):
        at = lax.rem(me + step, total)
        where = []
        for size in reversed(sizes):
            where.append(lax.rem(at, size))
            at = at // size
        return tuple(reversed(where))

    barrier = pltpu.get_barrier_semaphore()

    def greet(step, _):
        pl.semaphore_signal(barrier, inc=1, device_id=peer(step), device_id_type=pl.DeviceIdType.MESH)
        return 0

    lax.fori_loop(1, total, greet, 0)
    pl.semaphore_wait(barrier, total - 1)

    def send(step, _):
        pltpu.make_async_remote_copy(
            src_ref=stat,
            dst_ref=inbox.at[step - 1],
            send_sem=send_sem,
            recv_sem=recv_sem,
            device_id=peer(step),
            device_id_type=pl.DeviceIdType.MESH,
        ).start()
        return 0

    lax.fori_loop(1, total, send, 0)
    pltpu.make_async_copy(inbox, inbox, recv_sem).wait()
    sums = stat[...] + jnp.sum(inbox[...], axis=0)
    mean_sq = jnp.sum(sums[0:1], axis=1, keepdims=True) / jnp.sum(sums[1:2], axis=1, keepdims=True)
    out[...] = squared[...] / (mean_sq + 1e-06)
    pltpu.make_async_copy(inbox, inbox, send_sem).wait()


def shards(positions_now, velocities, positions_next, halo_counts, neighbour_lists, descendants):
    slots = positions_now.shape[-1]
    cx, cy, cz, width = neighbour_lists.shape
    cells = cx * cy * cz
    live = (
        jnp.arange(slots, dtype=jnp.int32)[None, None, None, :] < halo_counts[..., None]
    ).astype(jnp.float32)
    lv = live[:, :, :, None, :]
    tally = halo_counts[:, :, :, None, None].astype(jnp.float32)
    state = jnp.concatenate(
        [positions_now[:, :, :, :3, :], positions_now[:, :, :, 3:4, :] * lv, positions_next, jnp.broadcast_to(tally, lv.shape)], axis=3
    )
    below = shifted(state[-1:], "gx", 1)
    above = shifted(state[:1], "gx", -1)
    state = jnp.concatenate([below, state, above], axis=0)
    below = shifted(state[:, -1:], "gy", 1)
    above = shifted(state[:, :1], "gy", -1)
    state = jnp.concatenate([below, state, above], axis=1)
    if lax.axis_size("gz") == 2 and cz == 1:
        below = above = shifted(state, "gz", 1)
    else:
        below = shifted(state[:, :, -1:], "gz", 1)
        above = shifted(state[:, :, :1], "gz", -1)
    padded = jnp.concatenate([below, state, above], axis=2).reshape(-1, 8, slots)
    count = padded.shape[0]
    tallies = padded[:, 7, 0].astype(jnp.int32)
    drift, squared, stats = pl.pallas_call(
        functools.partial(kernel, (cx, cy, cz), width),
        out_shape=(
            jax.ShapeDtypeStruct((cells, 3, slots), jnp.float32),
            jax.ShapeDtypeStruct((cells, slots), jnp.float32),
            jax.ShapeDtypeStruct((8, slots), jnp.float32),
        ),
        in_specs=[pl.BlockSpec(memory_space=pltpu.SMEM)] * 2 + [pl.BlockSpec(memory_space=pltpu.VMEM)] * 3,
        out_specs=(pl.BlockSpec(memory_space=pltpu.VMEM),) * 3,
        scratch_shapes=[
            pltpu.VMEM((count, 8, slots), jnp.float32),
            pltpu.VMEM((width + SPAN + 1, 8, slots), jnp.float32),
        ],
    )(
        neighbour_lists.reshape(-1),
        tallies,
        padded,
        velocities.reshape(cells, 3, slots),
        descendants.reshape(cells, 2, slots),
    )
    axes = ("gx", "gy", "gz")
    sizes = tuple(lax.axis_size(name) for name in axes)
    peers = sizes[0] * sizes[1] * sizes[2] - 1
    tension = pl.pallas_call(
        functools.partial(scale_kernel, axes, sizes),
        out_shape=jax.ShapeDtypeStruct((cells, slots), jnp.float32),
        in_specs=[pl.BlockSpec(memory_space=pltpu.VMEM)] * 2,
        out_specs=pl.BlockSpec(memory_space=pltpu.VMEM),
        scratch_shapes=[
            pltpu.VMEM((peers, 8, slots), jnp.float32),
            pltpu.SemaphoreType.DMA,
            pltpu.SemaphoreType.DMA,
        ],
        compiler_params=pltpu.CompilerParams(collective_id=0, has_side_effects=True),
    )(stats, squared)
    return (drift.reshape(cx, cy, cz, 3, slots), tension.reshape(cx, cy, cz, slots))


def solution(mesh):
    return jax.shard_map(
        shards,
        mesh=mesh,
        in_specs=(
            P("gx", "gy", "gz", None, None),
            P("gx", "gy", "gz", None, None),
            P("gx", "gy", "gz", None, None),
            P("gx", "gy", "gz"),
            P("gx", "gy", "gz", None),
            P("gx", "gy", "gz", None, None),
        ),
        out_specs=(P("gx", "gy", "gz", None, None), P("gx", "gy", "gz", None)),
        check_vma=False,
    )
```

```python
import functools

import jax
import jax.numpy as jnp
from jax import lax
from jax.experimental import pallas as pl
from jax.experimental.pallas import tpu as pltpu
from jax.sharding import PartitionSpec as P

EPS_SQ = 0.01
STEP_DT = 0.3
HALF_KICK = 0.045
SPAN = 4


def shifted(shard, axis, by):
    peers = lax.axis_size(axis)
    return lax.ppermute(shard, axis, [(i, (i + by) % peers) for i in range(peers)])


def pieces(tile):
    first = tile.astype(jnp.bfloat16).astype(jnp.float32)
    rest = tile - first
    second = rest.astype(jnp.bfloat16).astype(jnp.float32)
    return first, second, rest - second


def kernel(dims, width, lists, padded, vel, desc, drift_ref, sq_ref, stat_ref, placed, packed, counts):
    cx, cy, cz = dims
    py, pz = cy + 2, cz + 2
    cells = cx * cy * cz
    slots = padded.shape[-1]
    row = lax.broadcasted_iota(jnp.int32, (8, slots), 0)
    lane = lax.broadcasted_iota(jnp.int32, (8, slots), 1)
    wide = SPAN * slots
    wrow = lax.broadcasted_iota(jnp.int32, (8, wide), 0)

    def place(n, _):
        ix, iy, iz = n // (py * pz), n // pz % py, n % pz
        fx = ix.astype(jnp.float32) - (cx + 2) / 2
        fy = iy.astype(jnp.float32) - (cy + 2) / 2
        fz = iz.astype(jnp.float32) - (cz + 2) / 2
        shift = jnp.where(row % 4 == 0, fx, jnp.where(row % 4 == 1, fy, jnp.where(row % 4 == 2, fz, 0.0)))
        tile = padded[n]
        placed[n] = tile + shift
        counts[n] = jnp.max(tile[7:8]).astype(jnp.int32)
        return 0

    lax.fori_loop(0, padded.shape[0], place, 0, unroll=6)

    def target(n, stats):
        ix, iy, iz = n // (cy * cz), n // cz % cy, n % cz
        corner = (ix * py + iy) * pz + iz
        base = corner + (py + 1) * pz + 1
        own = placed[base]
        count = counts[base]

        def source(k):
            code = lists[n * width + k]
            d9 = (code * 57) >> 9
            d3 = (code * 43) >> 7
            return corner + d9 * (py * pz) + (d3 - 3 * d9) * pz + code - 3 * d3

        at = jnp.int32(0)
        for k in range(width):
            cell = source(k)
            q, by = at // slots, at % slots
            turned = pltpu.roll(placed[cell], by, 1)
            packed[q] = jnp.where(lane >= by, turned, packed[q])
            packed[q + 1] = turned
            at = at + counts[cell]
        q, by = at // slots, at % slots
        packed[q] = jnp.where(lane >= by, 0.0, packed[q])
        for k in range(1, SPAN):
            packed[q + k] = jnp.zeros_like(own)
        chunks = (at + wide - 1) // wide

        norm = own[0:1] * own[0:1] + own[1:2] * own[1:2] + own[2:3] * own[2:3]
        ext = jnp.where(row < 3, -2.0 * own, jnp.where(row == 3, 1.0, jnp.where(row == 4, norm + EPS_SQ, 0.0)))
        a, b, c = pieces(ext)
        lhs = jnp.concatenate([a, b, c, a, b, a], axis=0).T.astype(jnp.bfloat16)

        def chunk(rows, m, acc):
            tile = jnp.concatenate([packed[m * SPAN + k] for k in range(SPAN)], axis=1)
            mass = tile[3:4]
            size = tile[0:1] * tile[0:1] + tile[1:2] * tile[1:2] + tile[2:3] * tile[2:3]
            x = jnp.where(wrow < 3, tile, jnp.where(wrow == 3, size, jnp.where(wrow == 4, 1.0, 0.0)))
            a, b, c = pieces(x)
            f = jnp.concatenate([a, a, a, b, b, c], axis=0).astype(jnp.bfloat16)
            mom = jnp.where(wrow < 3, tile * mass, jnp.where(wrow == 3, mass, 0.0))
            z = jnp.concatenate(list(pieces(mom)) + [jnp.zeros_like(mom)], axis=0).astype(jnp.bfloat16)
            dist_sq = jnp.dot(lhs[:rows], f, preferred_element_type=jnp.float32)
            inv = lax.rsqrt(dist_sq)
            weight = inv * inv * inv
            high = weight.astype(jnp.bfloat16)
            low = (weight - high.astype(jnp.float32)).astype(jnp.bfloat16)
            dn = (((1,), (1,)), ((), ()))
            acc += lax.dot_general(high, z, dn, preferred_element_type=jnp.float32)
            acc += lax.dot_general(low, z, dn, preferred_element_type=jnp.float32)
            return acc

        def attract(rows):
            acc = lax.fori_loop(
                0, chunks, functools.partial(chunk, rows), jnp.zeros((rows, 32), jnp.float32)
            )
            if rows < slots:
                acc = jnp.concatenate([acc, jnp.zeros((slots - rows, 32), jnp.float32)], axis=0)
            return acc

        acc = lax.cond(count > slots // 2, lambda: attract(slots), lambda: attract(slots // 2))
        acc = acc.T
        sums = acc[0:8] + acc[8:16] + acc[16:24]
        accel = sums[0:3] - own[0:3] * sums[3:4]
        predicted = own[0:3] + STEP_DT * vel[n] + HALF_KICK * accel
        links = desc[n]
        dcode = jnp.broadcast_to(links[0:1], (8, slots))
        dslot = jnp.broadcast_to(links[1:2], (8, slots))
        found = jnp.zeros((8, slots), jnp.float32)
        for code in range(27):
            near = corner + (code // 9) * py * pz + (code // 3 % 3) * pz + code % 3
            got = jnp.take_along_axis(placed[near], dslot, axis=1)
            found = jnp.where(dcode == code, got, found)
        live = lane[0:1] < count
        error = jnp.where(live, found[4:7] - predicted, 0.0)
        drift_ref[n] = error
        squared = jnp.sum(error * error, axis=0, keepdims=True)
        sq_ref[pl.ds(n, 1), :] = squared
        return stats + jnp.where(row == 0, squared, jnp.where((row == 1) & live, 1.0, 0.0))

    stat_ref[...] = lax.fori_loop(0, cells, target, jnp.zeros((8, slots), jnp.float32))[0:2]


def scale_kernel(axes, sizes, stat, squared, out, inbox, send_sem, recv_sem):
    total = 1
    me = 0
    for name, size in zip(axes, sizes):
        total *= size
        me = me * size + lax.axis_index(name)

    def peer(step):
        at = lax.rem(me + step, total)
        where = []
        for size in reversed(sizes):
            where.append(lax.rem(at, size))
            at = at // size
        return tuple(reversed(where))

    barrier = pltpu.get_barrier_semaphore()

    def greet(step, _):
        pl.semaphore_signal(barrier, inc=1, device_id=peer(step), device_id_type=pl.DeviceIdType.MESH)
        return 0

    lax.fori_loop(1, total, greet, 0)
    pl.semaphore_wait(barrier, total - 1)

    def send(step, _):
        pltpu.make_async_remote_copy(
            src_ref=stat,
            dst_ref=inbox.at[step - 1],
            send_sem=send_sem,
            recv_sem=recv_sem,
            device_id=peer(step),
            device_id_type=pl.DeviceIdType.MESH,
        ).start()
        return 0

    lax.fori_loop(1, total, send, 0)
    pltpu.make_async_copy(inbox, inbox, recv_sem).wait()
    sums = stat[...] + jnp.sum(inbox[...], axis=0)
    mean_sq = jnp.sum(sums[0:1], axis=1, keepdims=True) / jnp.sum(sums[1:2], axis=1, keepdims=True)
    out[...] = squared[...] / (mean_sq + 1e-06)
    pltpu.make_async_copy(inbox, inbox, send_sem).wait()


def shards(positions_now, velocities, positions_next, halo_counts, neighbour_lists, descendants):
    slots = positions_now.shape[-1]
    cx, cy, cz, width = neighbour_lists.shape
    cells = cx * cy * cz
    live = (
        jnp.arange(slots, dtype=jnp.int32)[None, None, None, :] < halo_counts[..., None]
    ).astype(jnp.float32)
    lv = live[:, :, :, None, :]
    tally = halo_counts[:, :, :, None, None].astype(jnp.float32)
    state = jnp.concatenate(
        [positions_now[:, :, :, :3, :], positions_now[:, :, :, 3:4, :] * lv, positions_next, jnp.broadcast_to(tally, lv.shape)], axis=3
    )
    below = shifted(state[-1:], "gx", 1)
    above = shifted(state[:1], "gx", -1)
    state = jnp.concatenate([below, state, above], axis=0)
    below = shifted(state[:, -1:], "gy", 1)
    above = shifted(state[:, :1], "gy", -1)
    state = jnp.concatenate([below, state, above], axis=1)
    if lax.axis_size("gz") == 2 and cz == 1:
        below = above = shifted(state, "gz", 1)
    else:
        below = shifted(state[:, :, -1:], "gz", 1)
        above = shifted(state[:, :, :1], "gz", -1)
    padded = jnp.concatenate([below, state, above], axis=2).reshape(-1, 8, slots)
    count = padded.shape[0]
    drift, squared, stats = pl.pallas_call(
        functools.partial(kernel, (cx, cy, cz), width),
        out_shape=(
            jax.ShapeDtypeStruct((cells, 3, slots), jnp.float32),
            jax.ShapeDtypeStruct((cells, slots), jnp.float32),
            jax.ShapeDtypeStruct((2, slots), jnp.float32),
        ),
        in_specs=[pl.BlockSpec(memory_space=pltpu.SMEM)] + [pl.BlockSpec(memory_space=pltpu.VMEM)] * 3,
        out_specs=(pl.BlockSpec(memory_space=pltpu.VMEM),) * 3,
        scratch_shapes=[
            pltpu.VMEM((count, 8, slots), jnp.float32),
            pltpu.VMEM((width + SPAN + 1, 8, slots), jnp.float32),
            pltpu.SMEM((count,), jnp.int32),
        ],
    )(
        neighbour_lists.reshape(-1),
        padded,
        velocities.reshape(cells, 3, slots),
        descendants.reshape(cells, 2, slots),
    )
    axes = ("gx", "gy", "gz")
    sizes = tuple(lax.axis_size(name) for name in axes)
    peers = sizes[0] * sizes[1] * sizes[2] - 1
    tension = pl.pallas_call(
        functools.partial(scale_kernel, axes, sizes),
        out_shape=jax.ShapeDtypeStruct((cells, slots), jnp.float32),
        in_specs=[pl.BlockSpec(memory_space=pltpu.VMEM)] * 2,
        out_specs=pl.BlockSpec(memory_space=pltpu.VMEM),
        scratch_shapes=[
            pltpu.VMEM((peers, 2, slots), jnp.float32),
            pltpu.SemaphoreType.DMA,
            pltpu.SemaphoreType.DMA,
        ],
        compiler_params=pltpu.CompilerParams(collective_id=0, has_side_effects=True),
    )(stats, squared)
    return (drift.reshape(cx, cy, cz, 3, slots), tension.reshape(cx, cy, cz, slots))


def solution(mesh):
    return jax.shard_map(
        shards,
        mesh=mesh,
        in_specs=(
            P("gx", "gy", "gz", None, None),
            P("gx", "gy", "gz", None, None),
            P("gx", "gy", "gz", None, None),
            P("gx", "gy", "gz"),
            P("gx", "gy", "gz", None),
            P("gx", "gy", "gz", None, None),
        ),
        out_specs=(P("gx", "gy", "gz", None, None), P("gx", "gy", "gz", None)),
        check_vma=False,
    )
```
